512 devices in a mesh: dp: 16 (over y_lo, x, core), ctx: 32 (over y_hi, z).
Axes of the slice: x: 4, y: 4 (y_hi: 2, y_lo: 2; y = y_hi * 2 + y_lo), z: 16, core: 2. Of those that a mesh axis runs over, the one named last changes fastest.
Arguments:
- grad_out: bfloat16 [65536, 4096], P(('dp', 'ctx')), may hold values from -24 to 24
- gate: bfloat16 [65536, 4096], P(('dp', 'ctx')), may hold values from -6 to 6
- conv_in: bfloat16 [65536, 4096], P(('dp', 'ctx')), may hold values from -6 to 6
- filt: bfloat16 [4096, 64], P('dp'), may hold values from -0.75 to 0.75
- doc_end: int32 [65536], P(('dp', 'ctx')), may hold values from 1 to 65536, as said below
Outputs:
- grad_in: bfloat16 [65536, 4096], P(('dp', 'ctx'))
- grad_filt: float32 [4096, 64], P('dp')
The draws below stay inside these ranges and needn't reach their ends.
Inputs may be any that keep to these rules, and one draw needn't show every extreme that they name: doc_end is the same for all rows of one document and larger than the row's own index; no document crosses a multiple of 4096.
All inputs are finite; a program needn't handle non-finite values.
Results may differ from the reference program's by a relative error of at most 0.0049.
Values may be sent and summed in bfloat16 or wider, within the bound.
A program may use at most 64 MiB of HBM per device.

```python
import jax
import jax.numpy as jnp
from jax import lax

C = 4096
TAPS = 64
TOK_DEV = 128
SEQ = 4096
TOKENS = 65536


def draw_doc_end(key, part):
    positions = jnp.arange(1, TOKENS + 1, dtype=jnp.int32)
    opening = jax.random.randint(key, (TOKENS,), 0, 2 * TOK_DEV) == 0
    opening = opening | (positions % SEQ == 0)
    candidate = jnp.where(opening, positions, TOKENS).astype(jnp.int32)
    return lax.cummin(candidate, axis=0, reverse=True)


def spiked(drawn, rng, source, target, shards_of, factor):
    def block_of(axis_at):
        return (jnp.arange(drawn.shape[axis_at]) // (drawn.shape[axis_at] // shards_of)).reshape((-1,) + (1,) * (drawn.ndim - 1 - axis_at))

    first = jax.random.permutation(rng, shards_of)[block_of(target)]
    far = (block_of(target) + shards_of // 2) % shards_of
    return jnp.where((block_of(source) == first) | (block_of(source) == far), factor * drawn, drawn)


def levels(stream_key, shape, pieces, least, high):
    def one(dim, shards_of):
        draws = jax.random.uniform(jax.random.fold_in(jax.random.fold_in(stream_key, 6), dim), (shards_of,), jnp.float32, least / len(pieces), high / len(pieces))
        return jnp.repeat(jnp.exp(draws), shape[dim] // shards_of).reshape((-1,) + (1,) * (len(shape) - dim - 1))

    level = one(*pieces[0])
    for cut in pieces[1:]:
        level = level * one(*cut)
    return level


def normal_values(rng, extent, scale, most, pieces=(), held_as=jnp.bfloat16):
    loudness = levels(rng, extent, pieces, -0.22, 0.18) if pieces else 1.0
    array = jax.random.normal(rng, extent, jnp.float32) * scale * loudness
    return jnp.minimum(jnp.maximum(array, -most), most).astype(held_as)


def bell_draw_with(key, extent, scale, limit, split, heavy, kind=jnp.bfloat16):
    values = scale * jax.random.normal(key, extent, jnp.float32)
    if split:
        values = values * levels(key, extent, split, -0.22, 0.18)
    return jnp.clip(spiked(values, jax.random.fold_in(key, 3), *heavy), -limit, limit).astype(kind)


def setup_inputs(seed: int = 0) -> dict:
    streams_of = jax.random.split(jax.random.key(seed), 6)
    grad_out = bell_draw_with(streams_of[0], (TOKENS, C), 1.0, 24.0, ((0, 512),), (0, 1, 512, 6.0))
    gate = normal_values(streams_of[1], (TOKENS, C), 1.0, 6.0, ((0, 512),))
    conv_in = normal_values(streams_of[2], (TOKENS, C), 1.0, 6.0, ((0, 512),))
    filt = normal_values(streams_of[3], (C, TAPS), TAPS ** -0.5, 0.75, ((0, 16),))
    doc_end = draw_doc_end(jax.random.fold_in(streams_of[5], 71), 0)
    return {"grad_out": grad_out, "gate": gate, "conv_in": conv_in, "filt": filt, "doc_end": doc_end}


def reference(grad_out, gate, conv_in, filt, doc_end):
    grad_y = (grad_out.astype(jnp.float32) * gate.astype(jnp.float32)).astype(jnp.bfloat16)
    padded = jnp.concatenate([grad_y, jnp.zeros((TAPS, C), jnp.bfloat16)], axis=0)
    filt_cols = filt.astype(jnp.float32).T
    offsets = jnp.arange(TAPS, dtype=jnp.int32)
    local_rows = jnp.arange(TOK_DEV, dtype=jnp.int32)

    def block(carry, which):
        first = (which * TOK_DEV).astype(jnp.int32)
        extended = lax.dynamic_slice_in_dim(padded, first, TOK_DEV + TAPS, 0)
        inputs = lax.dynamic_slice_in_dim(conv_in, first, TOK_DEV, 0).astype(jnp.float32)
        remaining = lax.dynamic_slice_in_dim(doc_end, first, TOK_DEV, 0) - (first + local_rows)
        windows = jax.vmap(lambda offset: lax.dynamic_slice_in_dim(extended, offset, TOK_DEV, 0))(offsets)
        in_document = offsets[:, None] < remaining[None, :]
        windows = jnp.where(in_document[:, :, None], windows.astype(jnp.float32), jnp.float32(0.0))
        grad_block = jnp.sum(windows * filt_cols[:, None, :], axis=0).astype(jnp.bfloat16)
        tap_block = jnp.sum(windows * inputs[None, :, :], axis=1)
        return carry + tap_block, grad_block

    total, grads = lax.scan(block, jnp.zeros((TAPS, C), jnp.float32), jnp.arange(TOKENS // TOK_DEV, dtype=jnp.int32))
    return grads.reshape(TOKENS, C), total.T
```

```python
import functools

import jax
import jax.numpy as jnp
from jax import lax
from jax.experimental import pallas as pl
from jax.experimental.pallas import tpu as pltpu
from jax.sharding import PartitionSpec as P

F32 = jnp.float32
BF16 = jnp.bfloat16
LANES = 128
SUB = 16
ROWS = 32
MESH = pl.DeviceIdType.MESH


def kernel(nz, doc_end, grad_out, gate, conv_in, taps_own, grad_in, grad_filt,
           go_v, gate_v, x_v, gy_v, halo_v, g_s, x_s, f_s, stage, limits, terms, taps_all, send, recv, zbuf, ybuf,
           o32, obuf, in_sem, halo_send, halo_recv, tap_send, tap_recv, rs_send, rs_recv,
           z_send, z_recv, y_send, y_recv, out_sem):
    rows, channels = go_v.shape
    half = gy_v.shape[1]
    taps = 2 * half
    tiles = channels // LANES
    owners = taps_all.shape[0]
    group = 2 * owners

    d = lax.axis_index("dp")
    c = lax.axis_index("ctx")
    yh = c // nz
    z = c % nz
    me = d * 2 + yh
    first_row = (d * (2 * nz) + c) * rows

    def plane_peer(q):
        return {"dp": q // 2, "ctx": (q % 2) * nz + z}

    def depth_peer(other):
        return {"ctx": yh * nz + other}

    before = {"ctx": (c + 2 * nz - 1) % (2 * nz)}
    after = {"ctx": (c + 1) % (2 * nz)}

    barrier = pltpu.get_barrier_semaphore()

    def greet_plane(k, carry):
        pl.semaphore_signal(barrier, inc=1, device_id=plane_peer((me + k) % group), device_id_type=MESH)
        return carry

    def greet_depth(k, carry):
        pl.semaphore_signal(barrier, inc=1, device_id=depth_peer((z + k) % nz), device_id_type=MESH)
        return carry

    pl.semaphore_signal(barrier, inc=1, device_id=before, device_id_type=MESH)
    pl.semaphore_signal(barrier, inc=1, device_id=after, device_id_type=MESH)
    lax.fori_loop(1, nz, greet_depth, 0)
    lax.fori_loop(1, group, greet_plane, 0)

    loads = []
    for part in range(2):
        rng = pl.ds(part * half * 2, half * 2)
        for which, (src, dst) in enumerate(((grad_out, go_v), (gate, gate_v), (conv_in, x_v))):
            loads.append(pltpu.make_async_copy(src.at[rng], dst.at[rng], in_sem.at[part * 3 + which]))
            loads[-1].start()

    def place(block, h, tile):
        at = (tile // SUB) * (16 * SUB) + h * 8 * SUB + tile % SUB
        stage[pl.ds(at, 8, stride=SUB), :] = block

    def settle(dst, base):
        at = pl.ds(pl.multiple_of(base * SUB, 16 * SUB), 16 * SUB)
        for side in range(2):
            dst[at, side * LANES:(side + 1) * LANES] = (
                stage[side * 16 * SUB:(side + 1) * 16 * SUB, :].astype(BF16))

    def spread(dst, base, blocks):
        for j, block in enumerate(blocks):
            for h in range(2):
                place(block[h * 8:(h + 1) * 8], h, j)
        settle(dst, base)

    def spread_inputs(a, carry, to_send):
        at = pl.multiple_of(a * 16, 16)
        blocks = []
        for j in range(tiles):
            cols = slice(j * LANES, (j + 1) * LANES)
            y = go_v[pl.ds(at, 16), cols].astype(F32) * gate_v[pl.ds(at, 16), cols].astype(F32)
            y = y.astype(BF16)
            if to_send:
                gy_v[a // 2, pl.ds(pl.multiple_of((a % 2) * 16, 16), 16), cols] = y
            blocks.append(y.astype(F32))
        spread(g_s, at, blocks)
        spread(x_s, at, [x_v[pl.ds(at, 16), j * LANES:(j + 1) * LANES].astype(F32) for j in range(tiles)])
        return carry

    width = 16 * SUB
    term = lax.broadcasted_iota(jnp.int32, (SUB, width), 1)
    kept = jnp.where(term % SUB == lax.broadcasted_iota(jnp.int32, (SUB, width), 0), 1.0, 0.0)
    place_of = (term // SUB).astype(F32)

    def reach(i):
        return (doc_end[i] - (first_row + i)).astype(F32)

    def fill_limits(ib, carry):
        v = jnp.zeros((SUB, width), F32)
        for r in range(16):
            v = jnp.where(term // SUB == r, reach(ib * 16 + r), v)
        limits[pl.ds(pl.multiple_of(ib * SUB, SUB), SUB), :] = v
        return carry

    lax.fori_loop(0, rows // 16, fill_limits, 0)

    for copy in loads[:3]:
        copy.wait()
    lax.fori_loop(0, rows // 32, functools.partial(spread_inputs, to_send=True), 0)
    for copy in loads[3:]:
        copy.wait()
    lax.fori_loop(rows // 32, rows // 16, functools.partial(spread_inputs, to_send=False), 0)

    pl.semaphore_wait(barrier, group - 1 + nz - 1 + 2)

    halos = []
    for part in range(2):
        halos.append(pltpu.make_async_remote_copy(
            src_ref=gy_v.at[part], dst_ref=halo_v.at[part], send_sem=halo_send.at[part],
            recv_sem=halo_recv.at[part], device_id=before, device_id_type=MESH))
        halos[-1].start()

    def tap_copy(peer, slot):
        return pltpu.make_async_remote_copy(
            src_ref=taps_own, dst_ref=taps_all.at[slot], send_sem=tap_send.at[peer],
            recv_sem=tap_recv.at[slot], device_id={"dp": peer}, device_id_type=MESH)

    def send_taps(k, carry):
        tap_copy((d + k) % owners, d).start()
        return carry

    lax.fori_loop(1, owners, send_taps, 0)
    taps_all[d] = taps_own[...]

    def tile_of(ref, index):
        return ref[pl.ds(pl.multiple_of(index * SUB, SUB), width), :]

    def add_to(ref, index, value):
        count = ref.shape[0] // (2 * SUB)
        for side in range(2):
            at = pl.ds(pl.multiple_of((side * count + index) * SUB, SUB), SUB)
            ref[at, :] = ref[at, :] + value[:, side * LANES:(side + 1) * LANES]

    def masked(inside):
        return jnp.where(inside, kept, 0.0).astype(BF16)

    def clear(ref):
        def one(k, carry):
            ref[pl.ds(pl.multiple_of(k * 32, 32), 32), :] = jnp.zeros((32, LANES), F32)
            return carry

        lax.fori_loop(0, ref.shape[0] // 32, one, 0)

    def filter_terms(low, high, part):
        def sixteen(ib, carry):
            xt = tile_of(x_s, ib * 16)
            limit = limits[pl.ds(pl.multiple_of(ib * SUB, SUB), SUB), :]
            for u in range(half):
                t = part * half + u
                product = tile_of(g_s, ib * 16 + t) * xt
                add_to(terms, t, jnp.dot(masked(limit > t), product, preferred_element_type=F32))
            return carry

        lax.fori_loop(low, high, sixteen, 0)

    def plane_copy(q, slot):
        return pltpu.make_async_remote_copy(
            src_ref=send.at[q], dst_ref=recv.at[slot], send_sem=rs_send.at[q],
            recv_sem=rs_recv.at[slot], device_id=plane_peer(q), device_id_type=MESH)

    def out_copy(a):
        rng = pl.ds(pl.multiple_of(a * 16, 16), 16)
        return pltpu.make_async_copy(obuf.at[rng], grad_in.at[rng], out_sem.at[a])

    def input_rows(chunk, carry):
        clear(o32)

        def sixteen_taps(tb, carry):
            ft = tile_of(f_s, tb * 16)
            tap = place_of + (tb * 16).astype(F32)
            for u in range(ROWS):
                i = chunk * ROWS + u
                product = tile_of(g_s, i + tb * 16) * ft
                add_to(o32, u, jnp.dot(masked(tap < reach(i)), product, preferred_element_type=F32))
            return carry

        lax.fori_loop(0, taps // 16, sixteen_taps, 0)
        for a in range(ROWS // 16):
            at = pl.multiple_of(chunk * ROWS + a * 16, 16)
            for j in range(tiles):
                base = ((j // SUB) * ROWS + a * 16) * SUB + j % SUB
                v = [o32[pl.ds(base + h * 8 * SUB, 8, stride=SUB), :] for h in range(2)]
                obuf[pl.ds(at, 16), j * LANES:(j + 1) * LANES] = jnp.concatenate(v, axis=0).astype(BF16)
        return carry

    clear(terms)
    cut = rows // 16 - half // 16
    filter_terms(0, cut, 0)
    filter_terms(0, cut - half // 16, 1)

    for part in range(2):
        halos[part].wait_recv()

        def spread_halo(a, carry):
            at = pl.multiple_of(a * 16, 16)
            spread(g_s, rows + part * half + at,
                   [halo_v[part, pl.ds(at, 16), j * LANES:(j + 1) * LANES].astype(F32) for j in range(tiles)])
            return carry

        lax.fori_loop(0, half // 16, spread_halo, 0)
        filter_terms(cut - part * (half // 16), rows // 16, part)

        def pack(p, carry):
            for jj in range(2):
                tile = p * 2 + jj
                for tg in range(half // 16):
                    base = ((tile // SUB) * taps + part * half + tg * 16) * SUB + tile % SUB
                    v = [terms[pl.ds(base + h * 8 * SUB, 8, stride=SUB), :] for h in range(2)]
                    send[p * 2 + part, tg * 16:(tg + 1) * 16, jj * LANES:(jj + 1) * LANES] = (
                        jnp.concatenate(v, axis=0).astype(BF16))
            return carry

        lax.fori_loop(0, owners, pack, 0)

        def send_terms(k, carry):
            q = ((d + k) % owners) * 2 + part

            @pl.when(q != me)
            def _():
                plane_copy(q, me).start()

            return carry

        lax.fori_loop(0, owners, send_terms, 0)

        if part == 0:
            def take_taps(k, carry):
                p = (d + k) % owners
                tap_copy(p, p).wait_recv()
                return carry

            lax.fori_loop(1, owners, take_taps, 0)

            def spread_taps(a, carry):
                at = pl.multiple_of(a * 16, 16)
                spread(f_s, at, [taps_all[j // 2, pl.ds(at, 16), (j % 2) * LANES:(j % 2 + 1) * LANES].astype(F32)
                                 for j in range(tiles)])
                return carry

            lax.fori_loop(0, taps // 16, spread_taps, 0)
            input_rows(0, 0)

    recv[me] = send[me]
    lax.fori_loop(1, 3, input_rows, 0)

    def take_terms(k, carry):
        s = (me + k) % group
        plane_copy(s, s).wait_recv()
        return carry

    lax.fori_loop(1, group, take_terms, 0)
    zero_half = jnp.zeros((half, recv.shape[2]), F32)
    summed = lax.fori_loop(0, group, lambda s, acc: acc + recv[s].astype(F32), zero_half)
    zbuf[z] = summed.astype(BF16)

    def depth_copy(other, slot):
        return pltpu.make_async_remote_copy(
            src_ref=zbuf.at[z], dst_ref=zbuf.at[slot], send_sem=z_send.at[other],
            recv_sem=z_recv.at[slot], device_id=depth_peer(other), device_id_type=MESH)

    def send_depth(k, carry):
        depth_copy((z + k) % nz, z).start()
        return carry

    lax.fori_loop(1, nz, send_depth, 0)
    lax.fori_loop(3, rows // ROWS, input_rows, 0)

    def take_depth(k, carry):
        other = (z + k) % nz
        depth_copy(other, other).wait_recv()
        return carry

    lax.fori_loop(1, nz, take_depth, 0)
    ybuf[yh] = lax.fori_loop(0, nz, lambda s, acc: acc + zbuf[s].astype(F32), zero_half)

    def swap_copy(slot):
        return pltpu.make_async_remote_copy(
            src_ref=ybuf.at[yh], dst_ref=ybuf.at[slot], send_sem=y_send, recv_sem=y_recv,
            device_id={"ctx": (1 - yh) * nz + z}, device_id_type=MESH)

    swap_copy(yh).start()

    def start_out(a, carry):
        out_copy(a).start()
        return carry

    lax.fori_loop(0, rows // 16, start_out, 0)
    swap_copy(1 - yh).wait_recv()
    grad_filt[0:half, :] = ybuf[0]
    grad_filt[half:taps, :] = ybuf[1]

    def end_out(a, carry):
        out_copy(a).wait()
        return carry

    lax.fori_loop(0, rows // 16, end_out, 0)
    for copy in halos:
        copy.wait_send()
    swap_copy(yh).wait_send()

    def end_taps(k, carry):
        tap_copy((d + k) % owners, d).wait_send()
        return carry

    def end_terms(k, carry):
        plane_copy((me + k) % group, me).wait_send()
        return carry

    def end_depth(k, carry):
        depth_copy((z + k) % nz, z).wait_send()
        return carry

    lax.fori_loop(1, owners, end_taps, 0)
    lax.fori_loop(1, group, end_terms, 0)
    lax.fori_loop(1, nz, end_depth, 0)


def body(grad_out, gate, conv_in, filt, doc_end):
    rows, channels = grad_out.shape
    owned, taps = filt.shape
    half = taps // 2
    owners = lax.axis_size("dp")
    nz = lax.axis_size("ctx") // 2
    group = 2 * owners
    any_space = pl.BlockSpec(memory_space=pl.ANY)
    vmem = pl.BlockSpec(memory_space=pltpu.VMEM)
    dma = pltpu.SemaphoreType.DMA
    grad_in, grad_filt = pl.pallas_call(
        functools.partial(kernel, nz),
        out_shape=(
            jax.ShapeDtypeStruct((rows, channels), BF16),
            jax.ShapeDtypeStruct((taps, owned), F32),
        ),
        in_specs=[pl.BlockSpec(memory_space=pltpu.SMEM), any_space, any_space, any_space, vmem],
        out_specs=(any_space, vmem),
        scratch_shapes=[
            pltpu.VMEM((rows, channels), BF16),
            pltpu.VMEM((rows, channels), BF16),
            pltpu.VMEM((rows, channels), BF16),
            pltpu.VMEM((2, half, channels), BF16),
            pltpu.VMEM((2, half, channels), BF16),
            pltpu.VMEM(((rows + taps) * SUB, 2 * LANES), BF16),
            pltpu.VMEM((rows * SUB, 2 * LANES), BF16),
            pltpu.VMEM((taps * SUB, 2 * LANES), BF16),
            pltpu.VMEM((2 * 16 * SUB, LANES), F32),
            pltpu.VMEM((rows, 16 * SUB), F32),
            pltpu.VMEM((2 * taps * SUB, LANES), F32),
            pltpu.VMEM((owners, taps, owned), BF16),
            pltpu.VMEM((group, half, owned), BF16),
            pltpu.VMEM((group, half, owned), BF16),
            pltpu.VMEM((nz, half, owned), BF16),
            pltpu.VMEM((2, half, owned), F32),
            pltpu.VMEM((2 * ROWS * SUB, LANES), F32),
            pltpu.VMEM((rows, channels), BF16),
            dma((6,)),
            dma((2,)),
            dma((2,)),
            dma((owners,)),
            dma((owners,)),
            dma((group,)),
            dma((group,)),
            dma((nz,)),
            dma((nz,)),
            dma,
            dma,
            dma((rows // 16,)),
        ],
        compiler_params=pltpu.CompilerParams(collective_id=0, has_side_effects=True),
        name="conv_backward",
    )(doc_end, grad_out, gate, conv_in, filt.T)
    return grad_in, grad_filt.T


def solution(mesh):
    placed = (
        P(("dp", "ctx"), None),
        P(("dp", "ctx"), None),
        P(("dp", "ctx"), None),
        P("dp", None),
        P(("dp", "ctx")),
    )
    return jax.shard_map(
        body,
        mesh=mesh,
        in_specs=placed,
        out_specs=(P(("dp", "ctx"), None), P("dp", None)),
        check_vma=False,
    )
```

```python
import functools

import jax
import jax.numpy as jnp
from jax import lax
from jax.experimental import pallas as pl
from jax.experimental.pallas import tpu as pltpu
from jax.sharding import PartitionSpec as P

F32 = jnp.float32
BF16 = jnp.bfloat16
LANES = 128
SUB = 16
ROWS = 32
MESH = pl.DeviceIdType.MESH


def kernel(nz, doc_end, grad_out, gate, conv_in, taps_own, grad_in, grad_filt,
           go_v, gate_v, x_v, gy_v, halo_v, g_s, x_s, f_s, stage, limits, terms, taps_all, send, pair, recv, zbuf, ybuf,
           o32, obuf, in_sem, halo_send, halo_recv, hand_send, hand_recv, tap_send, tap_recv, share_send,
           pair_send, pair_recv, rs_send, rs_recv,
           z_send, z_recv, y_send, y_recv, out_sem):
    rows, channels = go_v.shape
    half = gy_v.shape[1]
    taps = 2 * half
    tiles = channels // LANES
    owners = taps_all.shape[0]
    group = owners
    chips = owners // 2

    d = lax.axis_index("dp")
    c = lax.axis_index("ctx")
    yh = c // nz
    z = c % nz
    core = d % 2
    me = (d // 2) * 2 + yh
    first_row = (d * (2 * nz) + c) * rows

    def plane_peer(q):
        return {"dp": (q // 2) * 2 + core, "ctx": (q % 2) * nz + z}

    twin = {"dp": (d // 2) * 2 + 1 - core}

    def depth_peer(other):
        return {"ctx": yh * nz + other}

    last = 2 * nz - 1
    members = lax.axis_size("dp")
    across = (d + members // 2) % members
    hands_on = c == nz - 1
    before = {"dp": jnp.where(c == nz, across, d), "ctx": (c + last) % (last + 1)}
    after = {"dp": jnp.where(hands_on, across, d), "ctx": (c + 1) % (last + 1)}
    slot = jnp.where(hands_on, 1, 0)

    barrier = pltpu.get_barrier_semaphore()

    def greet_plane(k, carry):
        pl.semaphore_signal(barrier, inc=1, device_id=plane_peer((me + k) % group), device_id_type=MESH)
        return carry

    def greet_depth(k, carry):
        far = nz // 2 - k
        pl.semaphore_signal(barrier, inc=1, device_id=depth_peer((z + far) % nz), device_id_type=MESH)

        @pl.when(k > 0)
        def _():
            pl.semaphore_signal(barrier, inc=1, device_id=depth_peer((z + nz - far) % nz), device_id_type=MESH)

        return carry

    lax.fori_loop(0, nz // 2, greet_depth, 0)
    pl.semaphore_signal(barrier, inc=1, device_id=before, device_id_type=MESH)
    pl.semaphore_signal(barrier, inc=1, device_id=after, device_id_type=MESH)
    pl.semaphore_signal(barrier, inc=1, device_id=twin, device_id_type=MESH)
    lax.fori_loop(1, group, greet_plane, 0)

    loads = []
    for part in range(2):
        rng = pl.ds(part * half * 2, half * 2)
        for which, (src, dst) in enumerate(((grad_out, go_v), (gate, gate_v), (conv_in, x_v))):
            loads.append(pltpu.make_async_copy(src.at[rng], dst.at[rng], in_sem.at[part * 3 + which]))
            loads[-1].start()

    def place(block, h, tile):
        at = (tile // SUB) * (16 * SUB) + h * 8 * SUB + tile % SUB
        stage[pl.ds(at, 8, stride=SUB), :] = block

    def settle(dst, base):
        at = pl.ds(pl.multiple_of(base * SUB, 16 * SUB), 16 * SUB)
        for side in range(2):
            dst[at, side * LANES:(side + 1) * LANES] = (
                stage[side * 16 * SUB:(side + 1) * 16 * SUB, :].astype(BF16))

    def spread(dst, base, blocks):
        for j, block in enumerate(blocks):
            for h in range(2):
                place(block[h * 8:(h + 1) * 8], h, j)
        settle(dst, base)

    def spread_inputs(a, carry, to_send):
        at = pl.multiple_of(a * 16, 16)
        blocks = []
        for j in range(tiles):
            cols = slice(j * LANES, (j + 1) * LANES)
            y = go_v[pl.ds(at, 16), cols].astype(F32) * gate_v[pl.ds(at, 16), cols].astype(F32)
            y = y.astype(BF16)
            if to_send:
                gy_v[a // 2, pl.ds(pl.multiple_of((a % 2) * 16, 16), 16), cols] = y
            blocks.append(y.astype(F32))
        spread(g_s, at, blocks)
        spread(x_s, at, [x_v[pl.ds(at, 16), j * LANES:(j + 1) * LANES].astype(F32) for j in range(tiles)])
        return carry

    width = 16 * SUB
    term = lax.broadcasted_iota(jnp.int32, (SUB, width), 1)
    kept = jnp.where(term % SUB == lax.broadcasted_iota(jnp.int32, (SUB, width), 0), 1.0, 0.0)
    place_of = (term // SUB).astype(F32)

    def reach(i):
        return (doc_end[i] - (first_row + i)).astype(F32)

    def fill_limits(ib, carry):
        v = jnp.zeros((SUB, width), F32)
        for r in range(16):
            v = jnp.where(term // SUB == r, reach(ib * 16 + r), v)
        limits[pl.ds(pl.multiple_of(ib * SUB, SUB), SUB), :] = v
        return carry

    for copy in loads[:3]:
        copy.wait()
    lax.fori_loop(0, rows // 32, functools.partial(spread_inputs, to_send=True), 0)
    for copy in loads[3:]:
        copy.wait()
    lax.fori_loop(rows // 32, rows // 16, functools.partial(spread_inputs, to_send=False), 0)

    pl.semaphore_wait(barrier, group - 1 + 1 + nz - 1 + 2)

    pieces = taps // 8

    def piece(ref, k):
        return ref.at[k // (half // 8), pl.ds((k % (half // 8)) * 8, 8)]

    def halo_copy(k):
        return pltpu.make_async_remote_copy(
            src_ref=piece(gy_v, k), dst_ref=piece(halo_v.at[0], k), send_sem=halo_send.at[k],
            recv_sem=halo_recv.at[k], device_id=before, device_id_type=MESH)

    def hand_copy(k):
        return pltpu.make_async_remote_copy(
            src_ref=piece(halo_v.at[0], k), dst_ref=piece(halo_v.at[1], k), send_sem=hand_send.at[k],
            recv_sem=hand_recv.at[k], device_id={"dp": across}, device_id_type=MESH)

    def hand_on(low, high):
        @pl.when(hands_on)
        def _():
            for k in range(low, high):
                halo_copy(k).wait_recv()
                hand_copy(k).start()

    def take_halo(part):
        low, high = part * pieces // 2, (part + 1) * pieces // 2

        @pl.when(hands_on)
        def _():
            for k in range(low, high):
                hand_copy(k).wait_recv()

        @pl.when(jnp.logical_and(c != nz - 1, c < last))
        def _():
            for k in range(low, high):
                halo_copy(k).wait_recv()

        @pl.when(c == last)
        def _():
            halo_v[0, part] = jnp.zeros(halo_v.shape[2:], BF16)

    @pl.when(c > 0)
    def _():
        for k in range(pieces):
            halo_copy(k).start()

    def tap_copy(chip, slot_at):
        return pltpu.make_async_remote_copy(
            src_ref=taps_own, dst_ref=taps_all.at[slot_at], send_sem=tap_send.at[chip],
            recv_sem=tap_recv.at[slot_at], device_id={"dp": chip * 2 + core}, device_id_type=MESH)

    def own_tap_copy(slot_at):
        return pltpu.make_async_remote_copy(
            src_ref=taps_own, dst_ref=taps_all.at[slot_at], send_sem=tap_send.at[d // 2],
            recv_sem=tap_recv.at[slot_at], device_id=twin, device_id_type=MESH)

    def share_copy(slot_at):
        return pltpu.make_async_remote_copy(
            src_ref=taps_all.at[slot_at], dst_ref=taps_all.at[slot_at], send_sem=share_send.at[slot_at // 2],
            recv_sem=tap_recv.at[slot_at], device_id=twin, device_id_type=MESH)

    def other_chip(k):
        return (d // 2 + k) % chips

    def send_taps(k, carry):
        tap_copy(other_chip(k), d).start()
        return carry

    def share_taps(k, carry):
        p = other_chip(k) * 2 + core
        tap_copy(other_chip(k), p).wait_recv()
        share_copy(p).start()
        return carry

    lax.fori_loop(1, chips, send_taps, 0)
    own_tap_copy(d).start()
    taps_all[d] = taps_own[...]

    def tile_of(ref, index):
        return ref[pl.ds(pl.multiple_of(index * SUB, SUB), width), :]

    def add_to(ref, index, value):
        count = ref.shape[0] // (2 * SUB)
        for side in range(2):
            at = pl.ds(pl.multiple_of((side * count + index) * SUB, SUB), SUB)
            ref[at, :] = ref[at, :] + value[:, side * LANES:(side + 1) * LANES]

    def masked(inside):
        return jnp.where(inside, kept, 0.0).astype(BF16)

    def clear(ref):
        def one(k, carry):
            ref[pl.ds(pl.multiple_of(k * 32, 32), 32), :] = jnp.zeros((32, LANES), F32)
            return carry

        lax.fori_loop(0, ref.shape[0] // 32, one, 0)

    def filter_terms(low, high, part):
        def sixteen(ib, carry):
            xt = tile_of(x_s, ib * 16)
            limit = limits[pl.ds(pl.multiple_of(ib * SUB, SUB), SUB), :]
            for u in range(half):
                t = part * half + u
                product = tile_of(g_s, ib * 16 + t) * xt
                add_to(terms, t, jnp.dot(masked(limit > t), product, preferred_element_type=F32))
            return carry

        lax.fori_loop(low, high, sixteen, 0)

    def block_of(owner_core, part, chip):
        return (owner_core * 2 + part) * chips + chip

    def plane_copy(q, slot_at, part):
        return pltpu.make_async_remote_copy(
            src_ref=send.at[block_of(core, part, q // 2)], dst_ref=recv.at[slot_at], send_sem=rs_send.at[q],
            recv_sem=rs_recv.at[slot_at], device_id=plane_peer(q), device_id_type=MESH)

    def pair_copy(part):
        return pltpu.make_async_remote_copy(
            src_ref=send.at[pl.ds(block_of(1 - core, part, 0), chips)], dst_ref=pair.at[part],
            send_sem=pair_send.at[part], recv_sem=pair_recv.at[part], device_id=twin, device_id_type=MESH)

    def out_copy(a):
        rng = pl.ds(pl.multiple_of(a * 16, 16), 16)
        return pltpu.make_async_copy(obuf.at[rng], grad_in.at[rng], out_sem.at[a])

    def input_rows(chunk, carry):
        clear(o32)

        def sixteen_taps(tb, carry):
            ft = tile_of(f_s, tb * 16)
            tap = place_of + (tb * 16).astype(F32)
            for u in range(ROWS):
                i = chunk * ROWS + u
                product = tile_of(g_s, i + tb * 16) * ft
                add_to(o32, u, jnp.dot(masked(tap < reach(i)), product, preferred_element_type=F32))
            return carry

        lax.fori_loop(0, taps // 16, sixteen_taps, 0)
        for a in range(ROWS // 16):
            at = pl.multiple_of(chunk * ROWS + a * 16, 16)
            for j in range(tiles):
                base = ((j // SUB) * ROWS + a * 16) * SUB + j % SUB
                v = [o32[pl.ds(base + h * 8 * SUB, 8, stride=SUB), :] for h in range(2)]
                obuf[pl.ds(at, 16), j * LANES:(j + 1) * LANES] = jnp.concatenate(v, axis=0).astype(BF16)
        return carry

    lax.fori_loop(0, rows // 16, fill_limits, 0)
    clear(terms)
    cut = rows // 16 - half // 16
    filter_terms(0, cut, 0)
    lax.fori_loop(1, chips, share_taps, 0)
    hand_on(0, 2)
    filter_terms(0, cut - half // 16, 1)
    hand_on(2, 5)

    for part in range(2):
        take_halo(part)

        def spread_halo(a, carry):
            at = pl.multiple_of(a * 16, 16)
            spread(g_s, rows + part * half + at,
                   [halo_v[slot, part, pl.ds(at, 16), j * LANES:(j + 1) * LANES].astype(F32) for j in range(tiles)])
            return carry

        lax.fori_loop(0, half // 16, spread_halo, 0)
        filter_terms(cut - part * (half // 16), rows // 16, part)
        if part == 0:
            hand_on(5, pieces)

        def pack(chip, carry, owner_core):
            for jj in range(2):
                tile = chip * 4 + owner_core * 2 + jj
                for tg in range(half // 16):
                    base = ((tile // SUB) * taps + part * half + tg * 16) * SUB + tile % SUB
                    v = [terms[pl.ds(base + h * 8 * SUB, 8, stride=SUB), :] for h in range(2)]
                    send[block_of(owner_core, part, chip), tg * 16:(tg + 1) * 16,
                         jj * LANES:(jj + 1) * LANES] = jnp.concatenate(v, axis=0).astype(BF16)
            return carry

        lax.fori_loop(0, chips, functools.partial(pack, owner_core=1 - core), 0)
        pair_copy(part).start()
        lax.fori_loop(0, chips, functools.partial(pack, owner_core=core), 0)
        pair_copy(part).wait_recv()

        def add_terms(k, carry):
            chip = other_chip(k)
            at = block_of(core, part, chip)
            send[at] = (send[at].astype(F32) + pair[part, chip].astype(F32)).astype(BF16)
            return carry

        lax.fori_loop(0, chips, add_terms, 0)

        def start_terms(k, carry):
            q = other_chip(k) * 2 + part

            @pl.when(q != me)
            def _():
                plane_copy(q, me, part).start()

            return carry

        lax.fori_loop(0, chips, start_terms, 0)

        if part == 0:
            def take_taps(k, carry):
                share_copy(other_chip(k) * 2 + 1 - core).wait_recv()
                return carry

            lax.fori_loop(0, chips, take_taps, 0)

            def spread_taps(a, carry):
                at = pl.multiple_of(a * 16, 16)
                spread(f_s, at, [taps_all[j // 2, pl.ds(at, 16), (j % 2) * LANES:(j % 2 + 1) * LANES].astype(F32)
                                 for j in range(tiles)])
                return carry

            lax.fori_loop(0, taps // 16, spread_taps, 0)
            input_rows(0, 0)

    recv[me] = send[block_of(core, yh, d // 2)]
    lax.fori_loop(1, 3, input_rows, 0)

    def take_terms(k, carry):
        s = (me + k) % group
        plane_copy(s, s, yh).wait_recv()
        return carry

    lax.fori_loop(1, group, take_terms, 0)
    zero_half = jnp.zeros((half, recv.shape[2]), F32)
    summed = lax.fori_loop(0, group, lambda s, acc: acc + recv[s].astype(F32), zero_half)
    zbuf[z] = summed.astype(BF16)

    def depth_copy(other, slot):
        return pltpu.make_async_remote_copy(
            src_ref=zbuf.at[z], dst_ref=zbuf.at[slot], send_sem=z_send.at[other],
            recv_sem=z_recv.at[slot], device_id=depth_peer(other), device_id_type=MESH)

    def send_depth(k, carry):
        depth_copy((z + k) % nz, z).start()
        return carry

    lax.fori_loop(1, nz, send_depth, 0)
    lax.fori_loop(3, rows // ROWS, input_rows, 0)

    def take_depth(k, carry):
        other = (z + k) % nz
        depth_copy(other, other).wait_recv()
        return carry

    lax.fori_loop(1, nz, take_depth, 0)
    ybuf[yh] = lax.fori_loop(0, nz, lambda s, acc: acc + zbuf[s].astype(F32), zero_half)

    def swap_copy(slot):
        return pltpu.make_async_remote_copy(
            src_ref=ybuf.at[yh], dst_ref=ybuf.at[slot], send_sem=y_send, recv_sem=y_recv,
            device_id={"ctx": (1 - yh) * nz + z}, device_id_type=MESH)

    swap_copy(yh).start()

    def start_out(a, carry):
        out_copy(a).start()
        return carry

    lax.fori_loop(0, rows // 16, start_out, 0)
    swap_copy(1 - yh).wait_recv()
    grad_filt[0:half, :] = ybuf[0]
    grad_filt[half:taps, :] = ybuf[1]

    def end_out(a, carry):
        out_copy(a).wait()
        return carry

    lax.fori_loop(0, rows // 16, end_out, 0)
    @pl.when(c > 0)
    def _():
        for k in range(pieces):
            halo_copy(k).wait_send()

    @pl.when(hands_on)
    def _():
        for k in range(pieces):
            hand_copy(k).wait_send()

    swap_copy(yh).wait_send()

    def end_taps(k, carry):
        tap_copy(other_chip(k), d).wait_send()
        share_copy(other_chip(k) * 2 + core).wait_send()
        return carry

    def end_terms(k, carry):
        q = (me + k) % group
        plane_copy(q, me, q % 2).wait_send()
        return carry

    def end_depth(k, carry):
        depth_copy((z + k) % nz, z).wait_send()
        return carry

    lax.fori_loop(1, chips, end_taps, 0)
    own_tap_copy(d).wait_send()
    for part in range(2):
        pair_copy(part).wait_send()
    lax.fori_loop(1, group, end_terms, 0)
    lax.fori_loop(1, nz, end_depth, 0)


def body(grad_out, gate, conv_in, filt, doc_end):
    rows, channels = grad_out.shape
    owned, taps = filt.shape
    half = taps // 2
    owners = lax.axis_size("dp")
    nz = lax.axis_size("ctx") // 2
    any_space = pl.BlockSpec(memory_space=pl.ANY)
    vmem = pl.BlockSpec(memory_space=pltpu.VMEM)
    dma = pltpu.SemaphoreType.DMA
    grad_in, grad_filt = pl.pallas_call(
        functools.partial(kernel, nz),
        out_shape=(
            jax.ShapeDtypeStruct((rows, channels), BF16),
            jax.ShapeDtypeStruct((taps, owned), F32),
        ),
        in_specs=[pl.BlockSpec(memory_space=pltpu.SMEM), any_space, any_space, any_space, vmem],
        out_specs=(any_space, vmem),
        scratch_shapes=[
            pltpu.VMEM((rows, channels), BF16),
            pltpu.VMEM((rows, channels), BF16),
            pltpu.VMEM((rows, channels), BF16),
            pltpu.VMEM((2, half, channels), BF16),
            pltpu.VMEM((2, 2, half, channels), BF16),
            pltpu.VMEM(((rows + taps) * SUB, 2 * LANES), BF16),
            pltpu.VMEM((rows * SUB, 2 * LANES), BF16),
            pltpu.VMEM((taps * SUB, 2 * LANES), BF16),
            pltpu.VMEM((2 * 16 * SUB, LANES), F32),
            pltpu.VMEM((rows, 16 * SUB), F32),
            pltpu.VMEM((2 * taps * SUB, LANES), F32),
            pltpu.VMEM((owners, taps, owned), BF16),
            pltpu.VMEM((2 * owners, half, owned), BF16),
            pltpu.VMEM((2, owners // 2, half, owned), BF16),
            pltpu.VMEM((owners, half, owned), BF16),
            pltpu.VMEM((nz, half, owned), BF16),
            pltpu.VMEM((2, half, owned), F32),
            pltpu.VMEM((2 * ROWS * SUB, LANES), F32),
            pltpu.VMEM((rows, channels), BF16),
            dma((6,)),
            dma((taps // 8,)),
            dma((taps // 8,)),
            dma((taps // 8,)),
            dma((taps // 8,)),
            dma((owners // 2,)),
            dma((owners,)),
            dma((owners // 2,)),
            dma((2,)),
            dma((2,)),
            dma((owners,)),
            dma((owners,)),
            dma((nz,)),
            dma((nz,)),
            dma,
            dma,
            dma((rows // 16,)),
        ],
        compiler_params=pltpu.CompilerParams(collective_id=0, has_side_effects=True),
        name="conv_backward",
    )(doc_end, grad_out, gate, conv_in, filt.T)
    return grad_in, grad_filt.T


def solution(mesh):
    placed = (
        P(("dp", "ctx"), None),
        P(("dp", "ctx"), None),
        P(("dp", "ctx"), None),
        P("dp", None),
        P(("dp", "ctx")),
    )
    return jax.shard_map(
        body,
        mesh=mesh,
        in_specs=placed,
        out_specs=(P(("dp", "ctx"), None), P("dp", None)),
        check_vma=False,
    )
```

```python
import functools

import jax
import jax.numpy as jnp
from jax import lax
from jax.experimental import pallas as pl
from jax.experimental.pallas import tpu as pltpu
from jax.sharding import PartitionSpec as P

F32 = jnp.float32
BF16 = jnp.bfloat16
LANES = 128
SUB = 16
ROWS = 32
MESH = pl.DeviceIdType.MESH


def kernel(nz, doc_end, grad_out, gate, conv_in, taps_own, grad_in, grad_filt,
           go_v, gate_v, x_v, gy_v, halo_v, g_s, x_s, f_s, stage, limits, terms, taps_all, send, pair, recv, zbuf, ybuf,
           o32, obuf, in_sem, halo_send, halo_recv, hand_send, hand_recv, tap_send, tap_recv, share_send,
           pair_send, pair_recv, rs_send, rs_recv,
           z_send, z_recv, y_send, y_recv, out_sem):
    rows, channels = go_v.shape
    half = gy_v.shape[1]
    taps = 2 * half
    tiles = channels // LANES
    owners = taps_all.shape[0]
    group = owners
    chips = owners // 2

    d = lax.axis_index("dp")
    c = lax.axis_index("ctx")
    yh = c // nz
    z = c % nz
    core = d % 2
    me = (d // 2) * 2 + yh
    first_row = (d * (2 * nz) + c) * rows

    def plane_peer(q):
        return {"dp": (q // 2) * 2 + core, "ctx": (q % 2) * nz + z}

    twin = {"dp": (d // 2) * 2 + 1 - core}

    def depth_peer(other):
        return {"ctx": yh * nz + other}

    last = 2 * nz - 1
    members = lax.axis_size("dp")
    across = (d + members // 2) % members
    hands_on = c == nz - 1
    before = {"dp": jnp.where(c == nz, across, d), "ctx": (c + last) % (last + 1)}
    after = {"dp": jnp.where(hands_on, across, d), "ctx": (c + 1) % (last + 1)}
    slot = jnp.where(hands_on, 1, 0)

    barrier = pltpu.get_barrier_semaphore()

    def greet_plane(k, carry):
        pl.semaphore_signal(barrier, inc=1, device_id=plane_peer((me + k) % group), device_id_type=MESH)
        return carry

    def greet_depth(k, carry):
        far = nz // 2 - k
        pl.semaphore_signal(barrier, inc=1, device_id=depth_peer((z + far) % nz), device_id_type=MESH)

        @pl.when(k > 0)
        def _():
            pl.semaphore_signal(barrier, inc=1, device_id=depth_peer((z + nz - far) % nz), device_id_type=MESH)

        return carry

    lax.fori_loop(0, nz // 2, greet_depth, 0)
    pl.semaphore_signal(barrier, inc=1, device_id=before, device_id_type=MESH)
    pl.semaphore_signal(barrier, inc=1, device_id=after, device_id_type=MESH)
    pl.semaphore_signal(barrier, inc=1, device_id=twin, device_id_type=MESH)
    lax.fori_loop(1, group, greet_plane, 0)

    loads = []
    for part in range(2):
        rng = pl.ds(part * half * 2, half * 2)
        for which, (src, dst) in enumerate(((grad_out, go_v), (gate, gate_v), (conv_in, x_v))):
            loads.append(pltpu.make_async_copy(src.at[rng], dst.at[rng], in_sem.at[part * 3 + which]))
            loads[-1].start()

    def place(block, h, tile):
        at = (tile // SUB) * (16 * SUB) + h * 8 * SUB + tile % SUB
        stage[pl.ds(at, 8, stride=SUB), :] = block

    def settle(dst, base):
        at = pl.ds(pl.multiple_of(base * SUB, 16 * SUB), 16 * SUB)
        for side in range(2):
            dst[at, side * LANES:(side + 1) * LANES] = (
                stage[side * 16 * SUB:(side + 1) * 16 * SUB, :].astype(BF16))

    def spread(dst, base, blocks):
        for j, block in enumerate(blocks):
            for h in range(2):
                place(block[h * 8:(h + 1) * 8], h, j)
        settle(dst, base)

    def spread_inputs(a, carry, to_send):
        at = pl.multiple_of(a * 16, 16)
        blocks = []
        for j in range(tiles):
            cols = slice(j * LANES, (j + 1) * LANES)
            y = go_v[pl.ds(at, 16), cols].astype(F32) * gate_v[pl.ds(at, 16), cols].astype(F32)
            y = y.astype(BF16)
            if to_send:
                gy_v[a // 2, pl.ds(pl.multiple_of((a % 2) * 16, 16), 16), cols] = y
            blocks.append(y.astype(F32))
        spread(g_s, at, blocks)
        spread(x_s, at, [x_v[pl.ds(at, 16), j * LANES:(j + 1) * LANES].astype(F32) for j in range(tiles)])
        return carry

    width = 16 * SUB
    term = lax.broadcasted_iota(jnp.int32, (SUB, width), 1)
    kept = jnp.where(term % SUB == lax.broadcasted_iota(jnp.int32, (SUB, width), 0), 1.0, 0.0)
    place_of = (term // SUB).astype(F32)

    def reach(i):
        return (doc_end[i] - (first_row + i)).astype(F32)

    def fill_limits(ib, carry):
        v = jnp.zeros((SUB, width), F32)
        for r in range(16):
            v = jnp.where(term // SUB == r, reach(ib * 16 + r), v)
        limits[pl.ds(pl.multiple_of(ib * SUB, SUB), SUB), :] = v
        return carry

    for copy in loads[:3]:
        copy.wait()
    lax.fori_loop(0, rows // 32, functools.partial(spread_inputs, to_send=True), 0)
    for copy in loads[3:]:
        copy.wait()
    lax.fori_loop(rows // 32, rows // 16, functools.partial(spread_inputs, to_send=False), 0)

    pl.semaphore_wait(barrier, group - 1 + 1 + nz - 1 + 2)

    pieces = taps // 8

    def piece(ref, k):
        return ref.at[k // (half // 8), pl.ds((k % (half // 8)) * 8, 8)]

    def halo_copy(k):
        return pltpu.make_async_remote_copy(
            src_ref=piece(gy_v, k), dst_ref=piece(halo_v.at[0], k), send_sem=halo_send.at[k],
            recv_sem=halo_recv.at[k], device_id=before, device_id_type=MESH)

    def hand_copy(k):
        return pltpu.make_async_remote_copy(
            src_ref=piece(halo_v.at[0], k), dst_ref=piece(halo_v.at[1], k), send_sem=hand_send.at[k],
            recv_sem=hand_recv.at[k], device_id={"dp": across}, device_id_type=MESH)

    def hand_on(low, high):
        @pl.when(hands_on)
        def _():
            for k in range(low, high):
                halo_copy(k).wait_recv()
                hand_copy(k).start()

    def take_halo(part):
        low, high = part * pieces // 2, (part + 1) * pieces // 2

        @pl.when(hands_on)
        def _():
            for k in range(low, high):
                hand_copy(k).wait_recv()

        @pl.when(jnp.logical_and(c != nz - 1, c < last))
        def _():
            for k in range(low, high):
                halo_copy(k).wait_recv()

        @pl.when(c == last)
        def _():
            halo_v[0, part] = jnp.zeros(halo_v.shape[2:], BF16)

    @pl.when(c > 0)
    def _():
        for k in range(pieces):
            halo_copy(k).start()

    def tap_copy(chip, slot_at):
        return pltpu.make_async_remote_copy(
            src_ref=taps_own, dst_ref=taps_all.at[slot_at], send_sem=tap_send.at[chip],
            recv_sem=tap_recv.at[slot_at], device_id={"dp": chip * 2 + core}, device_id_type=MESH)

    def own_tap_copy(slot_at):
        return pltpu.make_async_remote_copy(
            src_ref=taps_own, dst_ref=taps_all.at[slot_at], send_sem=tap_send.at[d // 2],
            recv_sem=tap_recv.at[slot_at], device_id=twin, device_id_type=MESH)

    def share_copy(slot_at):
        return pltpu.make_async_remote_copy(
            src_ref=taps_all.at[slot_at], dst_ref=taps_all.at[slot_at], send_sem=share_send.at[slot_at // 2],
            recv_sem=tap_recv.at[slot_at], device_id=twin, device_id_type=MESH)

    def other_chip(k):
        return (d // 2 + k) % chips

    def send_taps(k, carry):
        tap_copy(other_chip(k), d).start()
        return carry

    def share_taps(k, carry):
        p = other_chip(k) * 2 + core
        tap_copy(other_chip(k), p).wait_recv()
        share_copy(p).start()
        return carry

    lax.fori_loop(1, chips, send_taps, 0)
    own_tap_copy(d).start()
    taps_all[d] = taps_own[...]

    def tile_of(ref, index):
        return ref[pl.ds(pl.multiple_of(index * SUB, SUB), width), :]

    def add_to(ref, index, value):
        count = ref.shape[0] // (2 * SUB)
        for side in range(2):
            at = pl.ds(pl.multiple_of((side * count + index) * SUB, SUB), SUB)
            ref[at, :] = ref[at, :] + value[:, side * LANES:(side + 1) * LANES]

    def masked(inside):
        return jnp.where(inside, kept, 0.0).astype(BF16)

    def clear(ref):
        def one(k, carry):
            ref[pl.ds(pl.multiple_of(k * 32, 32), 32), :] = jnp.zeros((32, LANES), F32)
            return carry

        lax.fori_loop(0, ref.shape[0] // 32, one, 0)

    def filter_terms(low, high, part):
        def sixteen(ib, carry):
            xt = tile_of(x_s, ib * 16)
            limit = limits[pl.ds(pl.multiple_of(ib * SUB, SUB), SUB), :]
            for u in range(half):
                t = part * half + u
                product = tile_of(g_s, ib * 16 + t) * xt
                add_to(terms, t, jnp.dot(masked(limit > t), product, preferred_element_type=F32))
            return carry

        lax.fori_loop(low, high, sixteen, 0)

    def block_of(owner_core, part, chip):
        return (owner_core * 2 + part) * chips + chip

    def plane_copy(q, slot_at, part):
        return pltpu.make_async_remote_copy(
            src_ref=send.at[block_of(core, part, q // 2)], dst_ref=recv.at[slot_at], send_sem=rs_send.at[q],
            recv_sem=rs_recv.at[slot_at], device_id=plane_peer(q), device_id_type=MESH)

    def pair_copy(part):
        return pltpu.make_async_remote_copy(
            src_ref=send.at[pl.ds(block_of(1 - core, part, 0), chips)], dst_ref=pair.at[part],
            send_sem=pair_send.at[part], recv_sem=pair_recv.at[part], device_id=twin, device_id_type=MESH)

    def out_copy(a):
        rng = pl.ds(pl.multiple_of(a * 16, 16), 16)
        return pltpu.make_async_copy(obuf.at[rng], grad_in.at[rng], out_sem.at[a])

    def out_rows(low, high):
        def start_out(a, carry):
            out_copy(a).start()
            return carry

        lax.fori_loop(low * (ROWS // 16), high * (ROWS // 16), start_out, 0)

    def input_rows(chunk, carry):
        clear(o32)

        def sixteen_taps(tb, carry):
            ft = tile_of(f_s, tb * 16)
            tap = place_of + (tb * 16).astype(F32)
            for u in range(ROWS):
                i = chunk * ROWS + u
                product = tile_of(g_s, i + tb * 16) * ft
                add_to(o32, u, jnp.dot(masked(tap < reach(i)), product, preferred_element_type=F32))
            return carry

        lax.fori_loop(0, taps // 16, sixteen_taps, 0)
        for a in range(ROWS // 16):
            at = pl.multiple_of(chunk * ROWS + a * 16, 16)
            for j in range(tiles):
                base = ((j // SUB) * ROWS + a * 16) * SUB + j % SUB
                v = [o32[pl.ds(base + h * 8 * SUB, 8, stride=SUB), :] for h in range(2)]
                obuf[pl.ds(at, 16), j * LANES:(j + 1) * LANES] = jnp.concatenate(v, axis=0).astype(BF16)
        return carry

    lax.fori_loop(0, rows // 16, fill_limits, 0)
    clear(terms)
    cut = rows // 16 - half // 16
    filter_terms(0, cut, 0)
    lax.fori_loop(1, chips, share_taps, 0)
    hand_on(0, 2)
    filter_terms(0, cut - half // 16, 1)
    hand_on(2, 5)

    for part in range(2):
        take_halo(part)

        def spread_halo(a, carry):
            at = pl.multiple_of(a * 16, 16)
            spread(g_s, rows + part * half + at,
                   [halo_v[slot, part, pl.ds(at, 16), j * LANES:(j + 1) * LANES].astype(F32) for j in range(tiles)])
            return carry

        lax.fori_loop(0, half // 16, spread_halo, 0)
        filter_terms(cut - part * (half // 16), rows // 16, part)
        if part == 0:
            hand_on(5, pieces)

        def pack(chip, carry, owner_core):
            for jj in range(2):
                tile = chip * 4 + owner_core * 2 + jj
                for tg in range(half // 16):
                    base = ((tile // SUB) * taps + part * half + tg * 16) * SUB + tile % SUB
                    v = [terms[pl.ds(base + h * 8 * SUB, 8, stride=SUB), :] for h in range(2)]
                    send[block_of(owner_core, part, chip), tg * 16:(tg + 1) * 16,
                         jj * LANES:(jj + 1) * LANES] = jnp.concatenate(v, axis=0).astype(BF16)
            return carry

        lax.fori_loop(0, chips, functools.partial(pack, owner_core=1 - core), 0)
        pair_copy(part).start()
        lax.fori_loop(0, chips, functools.partial(pack, owner_core=core), 0)
        pair_copy(part).wait_recv()

        def add_terms(k, carry):
            chip = other_chip(k)
            at = block_of(core, part, chip)
            send[at] = (send[at].astype(F32) + pair[part, chip].astype(F32)).astype(BF16)
            return carry

        lax.fori_loop(0, chips, add_terms, 0)

        def start_terms(k, carry):
            q = other_chip(k) * 2 + part

            @pl.when(q != me)
            def _():
                plane_copy(q, me, part).start()

            return carry

        lax.fori_loop(0, chips, start_terms, 0)

    recv[me] = send[block_of(core, yh, d // 2)]
    def take_taps(k, carry):
        share_copy(other_chip(k) * 2 + 1 - core).wait_recv()
        return carry

    lax.fori_loop(0, chips, take_taps, 0)

    def spread_taps(a, carry):
        at = pl.multiple_of(a * 16, 16)
        spread(f_s, at, [taps_all[j // 2, pl.ds(at, 16), (j % 2) * LANES:(j % 2 + 1) * LANES].astype(F32)
                         for j in range(tiles)])
        return carry

    lax.fori_loop(0, taps // 16, spread_taps, 0)
    input_rows(0, 0)

    def take_terms(k, carry):
        s = (me + k) % group
        plane_copy(s, s, yh).wait_recv()
        return carry

    lax.fori_loop(1, group, take_terms, 0)
    zero_half = jnp.zeros((half, recv.shape[2]), F32)
    summed = lax.fori_loop(0, group, lambda s, acc: acc + recv[s].astype(F32), zero_half)
    zbuf[z] = summed.astype(BF16)

    def depth_copy(other, slot):
        return pltpu.make_async_remote_copy(
            src_ref=zbuf.at[z], dst_ref=zbuf.at[slot], send_sem=z_send.at[other],
            recv_sem=z_recv.at[slot], device_id=depth_peer(other), device_id_type=MESH)

    def send_depth(k, carry):
        depth_copy((z + k) % nz, z).start()
        return carry

    lax.fori_loop(1, nz, send_depth, 0)
    lax.fori_loop(1, 3, input_rows, 0)
    out_rows(0, 2)

    def take_depth(k, carry):
        other = (z + k) % nz
        depth_copy(other, other).wait_recv()
        return carry

    lax.fori_loop(1, nz, take_depth, 0)
    ybuf[yh] = lax.fori_loop(0, nz, lambda s, acc: acc + zbuf[s].astype(F32), zero_half)

    def swap_copy(slot):
        return pltpu.make_async_remote_copy(
            src_ref=ybuf.at[yh], dst_ref=ybuf.at[slot], send_sem=y_send, recv_sem=y_recv,
            device_id={"ctx": (1 - yh) * nz + z}, device_id_type=MESH)

    swap_copy(yh).start()
    lax.fori_loop(3, rows // ROWS, input_rows, 0)
    out_rows(2, rows // ROWS)
    swap_copy(1 - yh).wait_recv()
    grad_filt[0:half, :] = ybuf[0]
    grad_filt[half:taps, :] = ybuf[1]

    def end_out(a, carry):
        out_copy(a).wait()
        return carry

    lax.fori_loop(0, rows // 16, end_out, 0)
    @pl.when(c > 0)
    def _():
        for k in range(pieces):
            halo_copy(k).wait_send()

    @pl.when(hands_on)
    def _():
        for k in range(pieces):
            hand_copy(k).wait_send()

    swap_copy(yh).wait_send()

    def end_taps(k, carry):
        tap_copy(other_chip(k), d).wait_send()
        share_copy(other_chip(k) * 2 + core).wait_send()
        return carry

    def end_terms(k, carry):
        q = (me + k) % group
        plane_copy(q, me, q % 2).wait_send()
        return carry

    def end_depth(k, carry):
        depth_copy((z + k) % nz, z).wait_send()
        return carry

    lax.fori_loop(1, chips, end_taps, 0)
    own_tap_copy(d).wait_send()
    for part in range(2):
        pair_copy(part).wait_send()
    lax.fori_loop(1, group, end_terms, 0)
    lax.fori_loop(1, nz, end_depth, 0)


def body(grad_out, gate, conv_in, filt, doc_end):
    rows, channels = grad_out.shape
    owned, taps = filt.shape
    half = taps // 2
    owners = lax.axis_size("dp")
    nz = lax.axis_size("ctx") // 2
    any_space = pl.BlockSpec(memory_space=pl.ANY)
    vmem = pl.BlockSpec(memory_space=pltpu.VMEM)
    dma = pltpu.SemaphoreType.DMA
    grad_in, grad_filt = pl.pallas_call(
        functools.partial(kernel, nz),
        out_shape=(
            jax.ShapeDtypeStruct((rows, channels), BF16),
            jax.ShapeDtypeStruct((taps, owned), F32),
        ),
        in_specs=[pl.BlockSpec(memory_space=pltpu.SMEM), any_space, any_space, any_space, vmem],
        out_specs=(any_space, vmem),
        scratch_shapes=[
            pltpu.VMEM((rows, channels), BF16),
            pltpu.VMEM((rows, channels), BF16),
            pltpu.VMEM((rows, channels), BF16),
            pltpu.VMEM((2, half, channels), BF16),
            pltpu.VMEM((2, 2, half, channels), BF16),
            pltpu.VMEM(((rows + taps) * SUB, 2 * LANES), BF16),
            pltpu.VMEM((rows * SUB, 2 * LANES), BF16),
            pltpu.VMEM((taps * SUB, 2 * LANES), BF16),
            pltpu.VMEM((2 * 16 * SUB, LANES), F32),
            pltpu.VMEM((rows, 16 * SUB), F32),
            pltpu.VMEM((2 * taps * SUB, LANES), F32),
            pltpu.VMEM((owners, taps, owned), BF16),
            pltpu.VMEM((2 * owners, half, owned), BF16),
            pltpu.VMEM((2, owners // 2, half, owned), BF16),
            pltpu.VMEM((owners, half, owned), BF16),
            pltpu.VMEM((nz, half, owned), BF16),
            pltpu.VMEM((2, half, owned), F32),
            pltpu.VMEM((2 * ROWS * SUB, LANES), F32),
            pltpu.VMEM((rows, channels), BF16),
            dma((6,)),
            dma((taps // 8,)),
            dma((taps // 8,)),
            dma((taps // 8,)),
            dma((taps // 8,)),
            dma((owners // 2,)),
            dma((owners,)),
            dma((owners // 2,)),
            dma((2,)),
            dma((2,)),
            dma((owners,)),
            dma((owners,)),
            dma((nz,)),
            dma((nz,)),
            dma,
            dma,
            dma((rows // 16,)),
        ],
        compiler_params=pltpu.CompilerParams(collective_id=0, has_side_effects=True),
        name="conv_backward",
    )(doc_end, grad_out, gate, conv_in, filt.T)
    return grad_in, grad_filt.T


def solution(mesh):
    placed = (
        P(("dp", "ctx"), None),
        P(("dp", "ctx"), None),
        P(("dp", "ctx"), None),
        P("dp", None),
        P(("dp", "ctx")),
    )
    return jax.shard_map(
        body,
        mesh=mesh,
        in_specs=placed,
        out_specs=(P(("dp", "ctx"), None), P("dp", None)),
        check_vma=False,
    )
```

```python
import functools

import jax
import jax.numpy as jnp
from jax import lax
from jax.experimental import pallas as pl
from jax.experimental.pallas import tpu as pltpu
from jax.sharding import PartitionSpec as P

F32 = jnp.float32
BF16 = jnp.bfloat16
LANES = 128
SUB = 16
ROWS = 32
MESH = pl.DeviceIdType.MESH


def kernel(nz, doc_end, grad_out, gate, conv_in, taps_own, grad_in, grad_filt,
           go_v, gate_v, x_v, gy_v, halo_v, g_s, x_s, f_s, stage, limits, terms, taps_all, send, pair, recv, zbuf, ybuf,
           o32, obuf, in_sem, halo_send, halo_recv, hand_send, hand_recv, tap_send, tap_recv, share_send,
           pair_send, pair_recv, rs_send, rs_recv,
           z_send, z_recv, y_send, y_recv, out_sem):
    rows, channels = go_v.shape
    half = gy_v.shape[1]
    taps = 2 * half
    tiles = channels // LANES
    owners = taps_all.shape[0]
    group = owners
    chips = owners // 2

    d = lax.axis_index("dp")
    c = lax.axis_index("ctx")
    yh = c // nz
    z = c % nz
    core = d % 2
    me = (d // 2) * 2 + yh
    first_row = (d * (2 * nz) + c) * rows

    def plane_peer(q):
        return {"dp": (q // 2) * 2 + core, "ctx": (q % 2) * nz + z}

    twin = {"dp": (d // 2) * 2 + 1 - core}

    def depth_peer(other):
        return {"ctx": yh * nz + other}

    last = 2 * nz - 1
    members = lax.axis_size("dp")
    across = (d + members // 2) % members
    hands_on = c == nz - 1
    before = {"dp": jnp.where(c == nz, across, d), "ctx": (c + last) % (last + 1)}
    after = {"dp": jnp.where(hands_on, across, d), "ctx": (c + 1) % (last + 1)}
    slot = jnp.where(hands_on, 1, 0)

    barrier = pltpu.get_barrier_semaphore()

    def greet_plane(k, carry):
        pl.semaphore_signal(barrier, inc=1, device_id=plane_peer((me + k) % group), device_id_type=MESH)
        return carry

    def greet_depth(k, carry):
        far = nz // 2 - k
        pl.semaphore_signal(barrier, inc=1, device_id=depth_peer((z + far) % nz), device_id_type=MESH)

        @pl.when(k > 0)
        def _():
            pl.semaphore_signal(barrier, inc=1, device_id=depth_peer((z + nz - far) % nz), device_id_type=MESH)

        return carry

    lax.fori_loop(0, nz // 2, greet_depth, 0)
    pl.semaphore_signal(barrier, inc=1, device_id=before, device_id_type=MESH)
    pl.semaphore_signal(barrier, inc=1, device_id=after, device_id_type=MESH)
    pl.semaphore_signal(barrier, inc=1, device_id=twin, device_id_type=MESH)
    lax.fori_loop(1, group, greet_plane, 0)

    loads = []
    for part in range(2):
        rng = pl.ds(part * half * 2, half * 2)
        for which, (src, dst) in enumerate(((grad_out, go_v), (gate, gate_v), (conv_in, x_v))):
            loads.append(pltpu.make_async_copy(src.at[rng], dst.at[rng], in_sem.at[part * 3 + which]))
            loads[-1].start()

    def place(block, h, tile):
        at = (tile // SUB) * (16 * SUB) + h * 8 * SUB + tile % SUB
        stage[pl.ds(at, 8, stride=SUB), :] = block

    def settle(dst, base):
        at = pl.ds(pl.multiple_of(base * SUB, 16 * SUB), 16 * SUB)
        for side in range(2):
            dst[at, side * LANES:(side + 1) * LANES] = (
                stage[side * 16 * SUB:(side + 1) * 16 * SUB, :].astype(BF16))

    def spread(dst, base, blocks):
        for j, block in enumerate(blocks):
            for h in range(2):
                place(block[h * 8:(h + 1) * 8], h, j)
        settle(dst, base)

    def spread_inputs(a, carry, to_send):
        at = pl.multiple_of(a * 16, 16)
        blocks = []
        for j in range(tiles):
            cols = slice(j * LANES, (j + 1) * LANES)
            y = go_v[pl.ds(at, 16), cols].astype(F32) * gate_v[pl.ds(at, 16), cols].astype(F32)
            y = y.astype(BF16)
            if to_send:
                gy_v[a // 2, pl.ds(pl.multiple_of((a % 2) * 16, 16), 16), cols] = y
            blocks.append(y.astype(F32))
        spread(g_s, at, blocks)
        spread(x_s, at, [x_v[pl.ds(at, 16), j * LANES:(j + 1) * LANES].astype(F32) for j in range(tiles)])
        return carry

    width = 16 * SUB
    term = lax.broadcasted_iota(jnp.int32, (SUB, width), 1)
    kept = jnp.where(term % SUB == lax.broadcasted_iota(jnp.int32, (SUB, width), 0), 1.0, 0.0)
    place_of = (term // SUB).astype(F32)

    def reach(i):
        return (doc_end[i] - (first_row + i)).astype(F32)

    def fill_limits(ib, carry):
        v = jnp.zeros((SUB, width), F32)
        for r in range(16):
            v = jnp.where(term // SUB == r, reach(ib * 16 + r), v)
        limits[pl.ds(pl.multiple_of(ib * SUB, SUB), SUB), :] = v
        return carry

    for copy in loads[:3]:
        copy.wait()
    lax.fori_loop(0, rows // 32, functools.partial(spread_inputs, to_send=True), 0)
    for copy in loads[3:]:
        copy.wait()
    lax.fori_loop(rows // 32, rows // 16, functools.partial(spread_inputs, to_send=False), 0)

    pl.semaphore_wait(barrier, group - 1 + 1 + nz - 1 + 2)

    pieces = taps // 8

    def piece(ref, k):
        return ref.at[k // (half // 8), pl.ds((k % (half // 8)) * 8, 8)]

    def halo_copy(k):
        return pltpu.make_async_remote_copy(
            src_ref=piece(gy_v, k), dst_ref=piece(halo_v.at[0], k), send_sem=halo_send.at[k],
            recv_sem=halo_recv.at[k], device_id=before, device_id_type=MESH)

    def hand_copy(k):
        return pltpu.make_async_remote_copy(
            src_ref=piece(halo_v.at[0], k), dst_ref=piece(halo_v.at[1], k), send_sem=hand_send.at[k],
            recv_sem=hand_recv.at[k], device_id={"dp": across}, device_id_type=MESH)

    def hand_on(low, high):
        @pl.when(hands_on)
        def _():
            for k in range(low, high):
                halo_copy(k).wait_recv()
                hand_copy(k).start()

    def take_halo(part):
        low, high = part * pieces // 2, (part + 1) * pieces // 2

        @pl.when(hands_on)
        def _():
            for k in range(low, high):
                hand_copy(k).wait_recv()

        @pl.when(jnp.logical_and(c != nz - 1, c < last))
        def _():
            for k in range(low, high):
                halo_copy(k).wait_recv()

        @pl.when(c == last)
        def _():
            halo_v[0, part] = jnp.zeros(halo_v.shape[2:], BF16)

    @pl.when(c > 0)
    def _():
        for k in range(pieces):
            halo_copy(k).start()

    def tap_copy(chip, slot_at):
        return pltpu.make_async_remote_copy(
            src_ref=taps_own, dst_ref=taps_all.at[slot_at], send_sem=tap_send.at[chip],
            recv_sem=tap_recv.at[slot_at], device_id={"dp": chip * 2 + core}, device_id_type=MESH)

    def own_tap_copy(slot_at):
        return pltpu.make_async_remote_copy(
            src_ref=taps_own, dst_ref=taps_all.at[slot_at], send_sem=tap_send.at[d // 2],
            recv_sem=tap_recv.at[slot_at], device_id=twin, device_id_type=MESH)

    def share_copy(slot_at):
        return pltpu.make_async_remote_copy(
            src_ref=taps_all.at[slot_at], dst_ref=taps_all.at[slot_at], send_sem=share_send.at[slot_at // 2],
            recv_sem=tap_recv.at[slot_at], device_id=twin, device_id_type=MESH)

    def other_chip(k):
        return (d // 2 + k) % chips

    def send_taps(k, carry):
        tap_copy(other_chip(k), d).start()
        return carry

    def share_taps(k, carry):
        p = other_chip(k) * 2 + core
        tap_copy(other_chip(k), p).wait_recv()
        share_copy(p).start()
        return carry

    lax.fori_loop(1, chips, send_taps, 0)
    own_tap_copy(d).start()
    taps_all[d] = taps_own[...]

    def tile_of(ref, index):
        return ref[pl.ds(pl.multiple_of(index * SUB, SUB), width), :]

    def add_to(ref, index, value):
        count = ref.shape[0] // (2 * SUB)
        for side in range(2):
            at = pl.ds(pl.multiple_of((side * count + index) * SUB, SUB), SUB)
            ref[at, :] = ref[at, :] + value[:, side * LANES:(side + 1) * LANES]

    def masked(inside):
        return jnp.where(inside, kept, 0.0).astype(BF16)

    def clear(ref):
        def one(k, carry):
            ref[pl.ds(pl.multiple_of(k * 32, 32), 32), :] = jnp.zeros((32, LANES), F32)
            return carry

        lax.fori_loop(0, ref.shape[0] // 32, one, 0)

    def filter_terms(low, high, part):
        def sixteen(ib, carry):
            xt = tile_of(x_s, ib * 16)
            limit = limits[pl.ds(pl.multiple_of(ib * SUB, SUB), SUB), :]
            for u in range(half):
                t = part * half + u
                product = tile_of(g_s, ib * 16 + t) * xt
                add_to(terms, t, jnp.dot(masked(limit > t), product, preferred_element_type=F32))
            return carry

        lax.fori_loop(low, high, sixteen, 0)

    def block_of(owner_core, part, chip):
        return (owner_core * 2 + part) * chips + chip

    def plane_copy(q, slot_at, part):
        return pltpu.make_async_remote_copy(
            src_ref=send.at[block_of(core, part, q // 2)], dst_ref=recv.at[slot_at], send_sem=rs_send.at[q],
            recv_sem=rs_recv.at[slot_at], device_id=plane_peer(q), device_id_type=MESH)

    def pair_copy(part):
        return pltpu.make_async_remote_copy(
            src_ref=send.at[pl.ds(block_of(1 - core, part, 0), chips)], dst_ref=pair.at[part],
            send_sem=pair_send.at[part], recv_sem=pair_recv.at[part], device_id=twin, device_id_type=MESH)

    def out_copy(a):
        rng = pl.ds(pl.multiple_of(a * 16, 16), 16)
        return pltpu.make_async_copy(obuf.at[rng], grad_in.at[rng], out_sem.at[a])

    def out_rows(low, high):
        def start_out(a, carry):
            out_copy(a).start()
            return carry

        lax.fori_loop(low * (ROWS // 16), high * (ROWS // 16), start_out, 0)

    def input_rows(chunk, carry):
        clear(o32)

        def sixteen_taps(tb, carry):
            ft = tile_of(f_s, tb * 16)
            tap = place_of + (tb * 16).astype(F32)
            for u in range(ROWS):
                i = chunk * ROWS + u
                product = tile_of(g_s, i + tb * 16) * ft
                add_to(o32, u, jnp.dot(masked(tap < reach(i)), product, preferred_element_type=F32))
            return carry

        lax.fori_loop(0, taps // 16, sixteen_taps, 0)
        for a in range(ROWS // 16):
            at = pl.multiple_of(chunk * ROWS + a * 16, 16)
            for j in range(tiles):
                base = ((j // SUB) * ROWS + a * 16) * SUB + j % SUB
                v = [o32[pl.ds(base + h * 8 * SUB, 8, stride=SUB), :] for h in range(2)]
                obuf[pl.ds(at, 16), j * LANES:(j + 1) * LANES] = jnp.concatenate(v, axis=0).astype(BF16)
        return carry

    lax.fori_loop(0, rows // 16, fill_limits, 0)
    clear(terms)
    cut = rows // 16 - half // 16
    filter_terms(0, cut, 0)
    lax.fori_loop(1, chips, share_taps, 0)
    hand_on(0, 2)
    filter_terms(0, cut - half // 16, 1)
    hand_on(2, 5)

    def finish(part):
        pair_copy(part).wait_recv()

        def add_terms(k, carry):
            chip = other_chip(k)
            at = block_of(core, part, chip)
            send[at] = (send[at].astype(F32) + pair[part, chip].astype(F32)).astype(BF16)
            return carry

        lax.fori_loop(0, chips, add_terms, 0)

        def start_terms(k, carry):
            q = other_chip(k) * 2 + part

            @pl.when(q != me)
            def _():
                plane_copy(q, me, part).start()

            return carry

        lax.fori_loop(0, chips, start_terms, 0)

    for part in range(2):
        take_halo(part)

        def spread_halo(a, carry):
            at = pl.multiple_of(a * 16, 16)
            spread(g_s, rows + part * half + at,
                   [halo_v[slot, part, pl.ds(at, 16), j * LANES:(j + 1) * LANES].astype(F32) for j in range(tiles)])
            return carry

        lax.fori_loop(0, half // 16, spread_halo, 0)
        if part == 1:
            filter_terms(cut - half // 16, cut, part)
            finish(0)
        filter_terms(cut, rows // 16, part)
        if part == 0:
            hand_on(5, pieces)

        def pack(chip, carry, owner_core):
            for jj in range(2):
                tile = chip * 4 + owner_core * 2 + jj
                for tg in range(half // 16):
                    base = ((tile // SUB) * taps + part * half + tg * 16) * SUB + tile % SUB
                    v = [terms[pl.ds(base + h * 8 * SUB, 8, stride=SUB), :] for h in range(2)]
                    send[block_of(owner_core, part, chip), tg * 16:(tg + 1) * 16,
                         jj * LANES:(jj + 1) * LANES] = jnp.concatenate(v, axis=0).astype(BF16)
            return carry

        lax.fori_loop(0, chips, functools.partial(pack, owner_core=1 - core), 0)
        pair_copy(part).start()
        lax.fori_loop(0, chips, functools.partial(pack, owner_core=core), 0)

    def take_taps(k, carry):
        share_copy(other_chip(k) * 2 + 1 - core).wait_recv()
        return carry

    lax.fori_loop(0, chips, take_taps, 0)

    def spread_taps(a, carry):
        at = pl.multiple_of(a * 16, 16)
        spread(f_s, at, [taps_all[j // 2, pl.ds(at, 16), (j % 2) * LANES:(j % 2 + 1) * LANES].astype(F32)
                         for j in range(tiles)])
        return carry

    lax.fori_loop(0, taps // 16, spread_taps, 0)
    finish(1)
    recv[me] = send[block_of(core, yh, d // 2)]
    input_rows(0, 0)

    def take_terms(k, carry):
        s = (me + k) % group
        plane_copy(s, s, yh).wait_recv()
        return carry

    lax.fori_loop(1, group, take_terms, 0)
    zero_half = jnp.zeros((half, recv.shape[2]), F32)
    summed = lax.fori_loop(0, group, lambda s, acc: acc + recv[s].astype(F32), zero_half)
    zbuf[z] = summed.astype(BF16)

    def depth_copy(other, slot):
        return pltpu.make_async_remote_copy(
            src_ref=zbuf.at[z], dst_ref=zbuf.at[slot], send_sem=z_send.at[other],
            recv_sem=z_recv.at[slot], device_id=depth_peer(other), device_id_type=MESH)

    def send_depth(k, carry):
        depth_copy((z + k) % nz, z).start()
        return carry

    lax.fori_loop(1, nz, send_depth, 0)
    lax.fori_loop(1, 3, input_rows, 0)
    out_rows(0, 2)

    def take_depth(k, carry):
        other = (z + k) % nz
        depth_copy(other, other).wait_recv()
        return carry

    lax.fori_loop(1, nz, take_depth, 0)
    ybuf[yh] = lax.fori_loop(0, nz, lambda s, acc: acc + zbuf[s].astype(F32), zero_half)

    def swap_copy(slot):
        return pltpu.make_async_remote_copy(
            src_ref=ybuf.at[yh], dst_ref=ybuf.at[slot], send_sem=y_send, recv_sem=y_recv,
            device_id={"ctx": (1 - yh) * nz + z}, device_id_type=MESH)

    swap_copy(yh).start()
    lax.fori_loop(3, rows // ROWS, input_rows, 0)
    out_rows(2, rows // ROWS)
    swap_copy(1 - yh).wait_recv()
    grad_filt[0:half, :] = ybuf[0]
    grad_filt[half:taps, :] = ybuf[1]

    def end_out(a, carry):
        out_copy(a).wait()
        return carry

    lax.fori_loop(0, rows // 16, end_out, 0)
    @pl.when(c > 0)
    def _():
        for k in range(pieces):
            halo_copy(k).wait_send()

    @pl.when(hands_on)
    def _():
        for k in range(pieces):
            hand_copy(k).wait_send()

    swap_copy(yh).wait_send()

    def end_taps(k, carry):
        tap_copy(other_chip(k), d).wait_send()
        share_copy(other_chip(k) * 2 + core).wait_send()
        return carry

    def end_terms(k, carry):
        q = (me + k) % group
        plane_copy(q, me, q % 2).wait_send()
        return carry

    def end_depth(k, carry):
        depth_copy((z + k) % nz, z).wait_send()
        return carry

    lax.fori_loop(1, chips, end_taps, 0)
    own_tap_copy(d).wait_send()
    for part in range(2):
        pair_copy(part).wait_send()
    lax.fori_loop(1, group, end_terms, 0)
    lax.fori_loop(1, nz, end_depth, 0)


def body(grad_out, gate, conv_in, filt, doc_end):
    rows, channels = grad_out.shape
    owned, taps = filt.shape
    half = taps // 2
    owners = lax.axis_size("dp")
    nz = lax.axis_size("ctx") // 2
    any_space = pl.BlockSpec(memory_space=pl.ANY)
    vmem = pl.BlockSpec(memory_space=pltpu.VMEM)
    dma = pltpu.SemaphoreType.DMA
    grad_in, grad_filt = pl.pallas_call(
        functools.partial(kernel, nz),
        out_shape=(
            jax.ShapeDtypeStruct((rows, channels), BF16),
            jax.ShapeDtypeStruct((taps, owned), F32),
        ),
        in_specs=[pl.BlockSpec(memory_space=pltpu.SMEM), any_space, any_space, any_space, vmem],
        out_specs=(any_space, vmem),
        scratch_shapes=[
            pltpu.VMEM((rows, channels), BF16),
            pltpu.VMEM((rows, channels), BF16),
            pltpu.VMEM((rows, channels), BF16),
            pltpu.VMEM((2, half, channels), BF16),
            pltpu.VMEM((2, 2, half, channels), BF16),
            pltpu.VMEM(((rows + taps) * SUB, 2 * LANES), BF16),
            pltpu.VMEM((rows * SUB, 2 * LANES), BF16),
            pltpu.VMEM((taps * SUB, 2 * LANES), BF16),
            pltpu.VMEM((2 * 16 * SUB, LANES), F32),
            pltpu.VMEM((rows, 16 * SUB), F32),
            pltpu.VMEM((2 * taps * SUB, LANES), F32),
            pltpu.VMEM((owners, taps, owned), BF16),
            pltpu.VMEM((2 * owners, half, owned), BF16),
            pltpu.VMEM((2, owners // 2, half, owned), BF16),
            pltpu.VMEM((owners, half, owned), BF16),
            pltpu.VMEM((nz, half, owned), BF16),
            pltpu.VMEM((2, half, owned), F32),
            pltpu.VMEM((2 * ROWS * SUB, LANES), F32),
            pltpu.VMEM((rows, channels), BF16),
            dma((6,)),
            dma((taps // 8,)),
            dma((taps // 8,)),
            dma((taps // 8,)),
            dma((taps // 8,)),
            dma((owners // 2,)),
            dma((owners,)),
            dma((owners // 2,)),
            dma((2,)),
            dma((2,)),
            dma((owners,)),
            dma((owners,)),
            dma((nz,)),
            dma((nz,)),
            dma,
            dma,
            dma((rows // 16,)),
        ],
        compiler_params=pltpu.CompilerParams(collective_id=0, has_side_effects=True),
        name="conv_backward",
    )(doc_end, grad_out, gate, conv_in, filt.T)
    return grad_in, grad_filt.T


def solution(mesh):
    placed = (
        P(("dp", "ctx"), None),
        P(("dp", "ctx"), None),
        P(("dp", "ctx"), None),
        P("dp", None),
        P(("dp", "ctx")),
    )
    return jax.shard_map(
        body,
        mesh=mesh,
        in_specs=placed,
        out_specs=(P(("dp", "ctx"), None), P("dp", None)),
        check_vma=False,
    )
```
